32 devices in a mesh: trial: 4 (over z), lat: 2 (over x), lon: 2 (over core), lev: 2 (over y).
Axes of the slice: x: 2, y: 2, z: 4, core: 2. Of those that a mesh axis runs over, the one named last changes fastest.
Arguments:
- density: float32 [32, 32, 256, 128], P(('trial', 'lat'), 'lon', 'lev'), parts along dimension 0, may hold values from 0.5 to 2
- crowding: float32 [32, 32, 256, 128], P(('trial', 'lat'), 'lon', 'lev'), parts along dimension 0, may hold values from 0.5 to 2
Outputs:
- scaled_field: float32 [32, 32, 256, 128], P(('trial', 'lat'), 'lon', 'lev'), parts along dimension 0
- density_end: float32 [32, 32, 256, 128], P(('trial', 'lat'), 'lon', 'lev'), parts along dimension 0
The draws below stay inside these ranges and needn't reach their ends.
There are 4 independent parts, one for each index of `trial`. The reference program is written for one: setup_inputs(seed, part) draws one part's arguments, and reference() takes and returns one part's arrays. A program takes and returns all parts, laid end to end along the dimension named above; each array names one. Nothing has to cross between parts.
All inputs are finite; a program needn't handle non-finite values.
Results may differ from the reference program's by a relative error of at most 0.000058.
Values sent between devices are 32-bit elements; how exact they have to be, the bound alone decides.
A program may use at most 64 MiB of HBM per device.

```python
import jax
import jax.numpy as jnp
from jax import lax

GRID_Y = 8
GRID_X = 32
GRID_Z = 256
SPECIES = 128
STEPS = 4


def shard_levels(stream_key, extent, cuts, least, largest):
    level, own = 1.0, jax.random.fold_in(stream_key, 6)
    for dim, blocks in cuts:
        draws = jnp.exp(jax.random.uniform(jax.random.fold_in(own, dim), (blocks,), jnp.float32, least / len(cuts), largest / len(cuts)))
        level = level * jnp.repeat(draws, extent[dim] // blocks).reshape([-1 if axis == dim else 1 for axis in range(len(extent))])
    return level


def setup_inputs(seed: int = 0, part: int = 0) -> dict:
    arg_keys = jax.random.split(jax.random.key(seed), 3)
    own_keys = jax.random.split(jax.random.fold_in(arg_keys[2], part), 3)
    density = jnp.clip(0.5 + 1.5 * jax.random.uniform(own_keys[0], (GRID_Y, GRID_X, GRID_Z, SPECIES), jnp.float32) ** shard_levels(own_keys[0], (GRID_Y, GRID_X, GRID_Z, SPECIES), ((0, 2), (1, 2), (2, 2)), -0.2, 0.2), 0.5, 2.0)
    crowding = jnp.clip(0.5 + 1.5 * jax.random.uniform(own_keys[1], (GRID_Y, GRID_X, GRID_Z, SPECIES), jnp.float32) ** shard_levels(own_keys[1], (GRID_Y, GRID_X, GRID_Z, SPECIES), ((0, 2), (1, 2), (2, 2)), -0.2, 0.2), 0.5, 2.0)
    return dict(density=density, crowding=crowding)


def inner_cells(values, dims):
    for dim in dims:
        values = lax.slice_in_dim(values, 1, values.shape[dim] - 1, axis=dim)
    return values

def side_cells(values, dim, start, dims):
    others = [other for other in dims if other != dim]
    values = inner_cells(values, others)
    return lax.slice_in_dim(values, start, start + values.shape[dim] - 2, axis=dim)

def advance(padded, crowding):
    middle = inner_cells(padded, (0, 1, 2))
    lower = [side_cells(padded, dim, 0, (0, 1, 2)) for dim in (0, 1, 2)]
    upper = [side_cells(padded, dim, 2, (0, 1, 2)) for dim in (0, 1, 2)]
    spread = lower[0] + upper[0] + lower[1] + upper[1] + lower[2] + upper[2] - 6.0 * middle
    return middle + 0.1 * spread + 0.2 * middle * (1.0 - middle * crowding)

def reference(density, crowding):
    for step in range(STEPS):
        density = advance(jnp.pad(density, ((1, 1), (1, 1), (1, 1), (0, 0)), mode='constant'), crowding)
    line_mean = lax.optimization_barrier(jnp.mean(density, axis=1, keepdims=True))
    centred = density - line_mean
    line_variance = lax.optimization_barrier(jnp.mean(centred * centred, axis=1, keepdims=True))
    scaled_field = centred * lax.rsqrt(line_variance + 0.0001)
    return (scaled_field, density)
```

```python
import functools

import jax
import jax.numpy as jnp
from jax import lax
from jax.experimental import pallas as pl
from jax.experimental.pallas import tpu as pltpu
from jax.sharding import PartitionSpec as P

STEPS = 4
PAD = 8
MESH = pl.DeviceIdType.MESH


def with_halo(cells, sides, width):
    for axis, dim in sides:
        count = lax.axis_size(axis)
        ends = count - 1
        head = lax.slice_in_dim(cells, 0, width, axis=dim)
        tail = lax.slice_in_dim(cells, cells.shape[dim] - width, cells.shape[dim], axis=dim)
        cells = jnp.concatenate(
            [
                lax.ppermute(tail, axis, [(i, (i + 1) % count) for i in range(ends)]),
                cells,
                lax.ppermute(head, axis, [((i + 1) % count, i) for i in range(ends)]),
            ],
            axis=dim,
        )
    return cells


def inner_cells(values, dims):
    for dim in dims:
        values = lax.slice_in_dim(values, 1, values.shape[dim] - 1, axis=dim)
    return values


def side_cells(values, dim, start, dims):
    others = [other for other in dims if other != dim]
    values = inner_cells(values, others)
    return lax.slice_in_dim(values, start, start + values.shape[dim] - 2, axis=dim)


def advance(padded, crowding):
    middle = inner_cells(padded, (0, 1, 2))
    lower = [side_cells(padded, dim, 0, (0, 1, 2)) for dim in (0, 1, 2)]
    upper = [side_cells(padded, dim, 2, (0, 1, 2)) for dim in (0, 1, 2)]
    spread = lower[0] + upper[0] + lower[1] + upper[1] + lower[2] + upper[2] - 6.0 * middle
    return middle + 0.1 * spread + 0.2 * middle * (1.0 - middle * crowding)


def general(density, crowding):
    for step in range(STEPS):
        padded = with_halo(density, (("lat", 0), ("lon", 1), ("lev", 2)), 1)
        density = advance(padded, crowding)
    count = density.shape[1] * lax.axis_size("lon")
    moved = density - 1.0
    totals, squares = lax.psum(
        (jnp.sum(moved, axis=1, keepdims=True), jnp.sum(moved * moved, axis=1, keepdims=True)),
        "lon",
    )
    line_mean = 1.0 + totals / count
    centred = density - line_mean
    line_variance = squares / count - totals / count * (totals / count)
    return (centred * lax.rsqrt(line_variance + 0.0001), density)


def tree_sum(terms):
    terms = list(terms)
    while len(terms) > 1:
        terms = [sum(terms[i : i + 2][1:], terms[i]) for i in range(0, len(terms), 2)]
    return terms[0]


def kernel(lons, levs, parts, dens, crowd, out_scaled, out_dens,
           field, cap, stats, peers, load_sem, face_send, face_recv,
           lon_send, lon_recv, lev_send, lev_recv, stat_send, stat_recv):
    rows, cols, deep, lanes = dens.shape
    size = deep // parts
    lat, lon, lev = lax.axis_index("lat"), lax.axis_index("lon"), lax.axis_index("lev")
    has_left, has_right = lon > 0, lon < lons - 1
    has_down, has_up = lev > 0, lev < levs - 1

    def place(r):
        return (1 - lat) * (rows - r) + lat * (r - 1)

    loads = []
    for r in range(1, rows + 1):
        loads.append(pltpu.make_async_copy(
            dens.at[place(r)],
            field.at[0, r, pl.ds(1, cols), pl.ds(PAD, deep)],
            load_sem.at[0, r - 1]))
        loads.append(pltpu.make_async_copy(
            crowd.at[place(r)], cap.at[r - 1], load_sem.at[1, r - 1]))
    for copy in loads:
        copy.start()

    barrier = pltpu.get_barrier_semaphore()
    pl.semaphore_signal(barrier, inc=1, device_id={"lat": 1 - lat}, device_id_type=MESH)
    for j in range(1, lons):
        pl.semaphore_signal(barrier, inc=1, device_id={"lon": lax.rem(lon + j, lons)}, device_id_type=MESH)
    if levs > 1:
        @pl.when(has_down)
        def _():
            pl.semaphore_signal(barrier, inc=1, device_id={"lev": lev - 1}, device_id_type=MESH)

        @pl.when(has_up)
        def _():
            pl.semaphore_signal(barrier, inc=1, device_id={"lev": lev + 1}, device_id_type=MESH)
    pl.semaphore_wait(barrier, lons + has_down.astype(jnp.int32) + has_up.astype(jnp.int32))

    def face(t, k):
        if t == 0:
            src = dens.at[place(1), :, pl.ds(k * size, size)]
        else:
            src = field.at[t, 1, pl.ds(1, cols), pl.ds(PAD + k * size, size)]
        return pltpu.make_async_remote_copy(
            src_ref=src,
            dst_ref=field.at[t, 0, pl.ds(1, cols), pl.ds(PAD + k * size, size)],
            send_sem=face_send.at[t, k],
            recv_sem=face_recv.at[t, k],
            device_id={"lat": 1 - lat},
            device_id_type=MESH,
        )

    def lon_side(t, right):
        own, theirs = (cols, 0) if right else (1, cols + 1)
        span = pl.ds(1, rows)
        return pltpu.make_async_remote_copy(
            src_ref=field.at[t, span, own, pl.ds(PAD, deep)],
            dst_ref=field.at[t, span, theirs, pl.ds(PAD, deep)],
            send_sem=lon_send.at[t, int(right)],
            recv_sem=lon_recv.at[t, int(right)],
            device_id={"lon": lon + 1 if right else lon - 1},
            device_id_type=MESH,
        )

    def lev_side(t, up):
        own, theirs = (PAD + deep - 1, PAD - 1) if up else (PAD, PAD + deep)
        span = (pl.ds(1, rows), pl.ds(1, cols))
        return pltpu.make_async_remote_copy(
            src_ref=field.at[t, span[0], span[1], pl.ds(own, 1)],
            dst_ref=field.at[t, span[0], span[1], pl.ds(theirs, 1)],
            send_sem=lev_send.at[t, int(up)],
            recv_sem=lev_recv.at[t, int(up)],
            device_id={"lev": lev + 1 if up else lev - 1},
            device_id_type=MESH,
        )

    def sides(t, act):
        if lons > 1:
            pl.when(has_right)(lambda: act(lon_side(t, True), 1))
            pl.when(has_left)(lambda: act(lon_side(t, False), 0))
        if levs > 1:
            pl.when(has_up)(lambda: act(lev_side(t, True), 1))
            pl.when(has_down)(lambda: act(lev_side(t, False), 0))

    def start_sides(t):
        sides(t, lambda copy, _: copy.start())

    def wait_sides_sent(t):
        sides(t, lambda copy, _: copy.wait_send())

    def wait_sides(t):
        if lons > 1:
            pl.when(has_left)(lambda: lon_side(t, True).wait_recv())
            pl.when(has_right)(lambda: lon_side(t, False).wait_recv())
        if levs > 1:
            pl.when(has_down)(lambda: lev_side(t, True).wait_recv())
            pl.when(has_up)(lambda: lev_side(t, False).wait_recv())

    def stat(part, j):
        if part < parts:
            pick = (0, slice(None), pl.ds(part * size, size))
        else:
            pick = (pl.ds(1, rows - 1),)
        return pltpu.make_async_remote_copy(
            src_ref=stats.at[pick],
            dst_ref=peers.at[(j - 1,) + pick],
            send_sem=stat_send.at[part, j - 1],
            recv_sem=stat_recv.at[part, j - 1],
            device_id={"lon": lax.rem(lon + j, lons)},
            device_id_type=MESH,
        )

    for k in range(parts):
        face(0, k).start()

    def clear_cols(at):
        for t in range(STEPS):
            def row(i, _, t=t):
                field[t, i, at, pl.ds(PAD, deep)] = jnp.zeros((deep, lanes), jnp.float32)
                return 0
            lax.fori_loop(1, rows + 1, row, 0)

    def clear_level(at):
        for t in range(STEPS):
            def row(i, _, t=t):
                def col(c, _):
                    field[t, i, c, pl.ds(at, PAD)] = jnp.zeros((PAD, lanes), jnp.float32)
                    return 0
                return lax.fori_loop(1, cols + 1, col, 0)
            lax.fori_loop(1, rows + 1, row, 0)

    pl.when(jnp.logical_not(has_left))(lambda: clear_cols(0))
    pl.when(jnp.logical_not(has_right))(lambda: clear_cols(cols + 1))
    pl.when(jnp.logical_not(has_down))(lambda: clear_level(0))
    pl.when(jnp.logical_not(has_up))(lambda: clear_level(PAD + deep))

    for copy in loads:
        copy.wait()
    start_sides(0)

    def cell(t, r, c, at, span, last):
        here = field[t, r, c, pl.ds(PAD + at, span)]
        near = (field[t, r, c - 1, pl.ds(PAD + at, span)] + field[t, r, c + 1, pl.ds(PAD + at, span)])
        near += (field[t, r, c, pl.ds(PAD - 1 + at, span)] + field[t, r, c, pl.ds(PAD + 1 + at, span)])
        near += field[t, r - 1, c, pl.ds(PAD + at, span)]
        if not last:
            near += field[t, r + 1, c, pl.ds(PAD + at, span)]
        limit = cap[r - 1, c - 1, pl.ds(at, span)]
        return here * (0.6 - 0.2 * (here * limit)) + 0.1 * near

    def advance_row(t, r, at, span, last):
        def col(c, _):
            field[t + 1, r, c, pl.ds(PAD + at, span)] = cell(t, r, c, at, span, last)
            return 0
        lax.fori_loop(1, cols + 1, col, 0)

    for t in range(STEPS - 1):
        wait_sides(t)

        def inner(r, _, t=t):
            advance_row(t, r, 0, deep, False)
            return 0

        lax.fori_loop(2, rows, inner, 0)
        advance_row(t, rows, 0, deep, True)
        for k in range(parts):
            face(t, k).wait_recv()
            advance_row(t, 1, k * size, size, rows == 1)
            face(t + 1, k).start()
        start_sides(t + 1)

    t = STEPS - 1
    wait_sides(t)

    def finish(r, at, last):
        values = [cell(t, r, c, at, 8, last) for c in range(1, cols + 1)]
        for c in range(cols):
            out_dens[place(r), c, pl.ds(at, 8)] = values[c]
        total = tree_sum(values)
        mean = total * (1.0 / cols)
        stats[r - 1, 0, pl.ds(at, 8)] = total
        stats[r - 1, 1, pl.ds(at, 8)] = tree_sum([(v - mean) * (v - mean) for v in values])

    def scale(r, at):
        pair = [(stats[r - 1, 0, pl.ds(at, 8)], stats[r - 1, 1, pl.ds(at, 8)])]
        for j in range(lons - 1):
            pair.append((peers[j, r - 1, 0, pl.ds(at, 8)], peers[j, r - 1, 1, pl.ds(at, 8)]))
        count = cols * lons
        mean = tree_sum([p[0] for p in pair]) * (1.0 / count)
        square = tree_sum([p[1] + cols * (p[0] * (1.0 / cols) - mean) ** 2 for p in pair])
        gain = lax.rsqrt(square * (1.0 / count) + 0.0001)
        for c in range(cols):
            out_scaled[place(r), c, pl.ds(at, 8)] = (out_dens[place(r), c, pl.ds(at, 8)] - mean) * gain

    def tiles(first, many, act):
        def tile(i, _):
            act(pl.multiple_of(i * 8, 8))
            return 0
        lax.fori_loop(first // 8, (first + many) // 8, tile, 0)

    def each_inner(act):
        def row(r, _):
            tiles(0, deep, lambda at: act(r, at))
            return 0
        lax.fori_loop(2, rows, row, 0)

    each_inner(lambda r, at: finish(r, at, False))
    tiles(0, deep, lambda at: finish(rows, at, True))
    for j in range(1, lons):
        stat(parts, j).start()
    for k in range(parts):
        face(t, k).wait_recv()
        tiles(k * size, size, lambda at: finish(1, at, False))
        for j in range(1, lons):
            stat(k, j).start()
        if k == 0:
            for j in range(1, lons):
                stat(parts, j).wait_recv()
            each_inner(scale)
            tiles(0, deep, lambda at: scale(rows, at))
        else:
            for j in range(1, lons):
                stat(k - 1, j).wait_recv()
            tiles((k - 1) * size, size, lambda at: scale(1, at))
    for s in range(STEPS):
        for k in range(parts):
            face(s, k).wait_send()
        wait_sides_sent(s)
    for j in range(1, lons):
        stat(parts - 1, j).wait_recv()
    tiles((parts - 1) * size, size, lambda at: scale(1, at))
    for j in range(1, lons):
        for part in range(parts + 1):
            stat(part, j).wait_send()


def one_kernel(lons, levs, density, crowding):
    rows, cols, deep, lanes = density.shape
    parts = 4
    sem = pltpu.SemaphoreType.DMA
    peers = max(lons - 1, 1)
    out = pltpu.VMEM(density.shape, jnp.float32)
    return pl.pallas_call(
        functools.partial(kernel, lons, levs, parts),
        out_shape=(out, out),
        in_specs=[pl.BlockSpec(memory_space=pl.ANY)] * 2,
        out_specs=[pl.BlockSpec(memory_space=pltpu.VMEM)] * 2,
        scratch_shapes=[
            pltpu.VMEM((STEPS, rows + 1, cols + 2, deep + 2 * PAD, lanes), jnp.float32),
            pltpu.VMEM((rows, cols, deep, lanes), jnp.float32),
            pltpu.VMEM((rows, 2, deep, lanes), jnp.float32),
            pltpu.VMEM((peers, rows, 2, deep, lanes), jnp.float32),
            sem((2, rows)),
            sem((STEPS, parts)),
            sem((STEPS, parts)),
            sem((STEPS, 2)),
            sem((STEPS, 2)),
            sem((STEPS, 2)),
            sem((STEPS, 2)),
            sem((parts + 1, peers)),
            sem((parts + 1, peers)),
        ],
        compiler_params=pltpu.CompilerParams(
            collective_id=0, has_side_effects=True, vmem_limit_bytes=VMEM_LIMIT
        ),
    )(density, crowding)


VMEM_LIMIT = 44 * 2**20


def solution(mesh):
    lats, lons, levs = mesh.shape["lat"], mesh.shape["lon"], mesh.shape["lev"]

    def shards(density, crowding):
        rows, cols, deep, lanes = density.shape
        words = lanes * (
            STEPS * (rows + 1) * (cols + 2) * (deep + 2 * PAD)
            + 3 * rows * cols * deep
            + 2 * lons * rows * deep
        )
        fits = lats == 2 and rows > 1 and lanes == 128 and deep % 32 == 0 and 4 * words < VMEM_LIMIT
        if fits:
            return tuple(one_kernel(lons, levs, density, crowding))
        return general(density, crowding)

    spec = P(("trial", "lat"), "lon", "lev", None)
    return jax.shard_map(
        shards, mesh=mesh, in_specs=(spec, spec), out_specs=(spec, spec), check_vma=False
    )
```

```python
import functools

import jax
import jax.numpy as jnp
from jax import lax
from jax.experimental import pallas as pl
from jax.experimental.pallas import tpu as pltpu
from jax.sharding import PartitionSpec as P

STEPS = 4
PAD = 8
MESH = pl.DeviceIdType.MESH


def with_halo(cells, sides, width):
    for axis, dim in sides:
        count = lax.axis_size(axis)
        ends = count - 1
        head = lax.slice_in_dim(cells, 0, width, axis=dim)
        tail = lax.slice_in_dim(cells, cells.shape[dim] - width, cells.shape[dim], axis=dim)
        cells = jnp.concatenate(
            [
                lax.ppermute(tail, axis, [(i, (i + 1) % count) for i in range(ends)]),
                cells,
                lax.ppermute(head, axis, [((i + 1) % count, i) for i in range(ends)]),
            ],
            axis=dim,
        )
    return cells


def inner_cells(values, dims):
    for dim in dims:
        values = lax.slice_in_dim(values, 1, values.shape[dim] - 1, axis=dim)
    return values


def side_cells(values, dim, start, dims):
    others = [other for other in dims if other != dim]
    values = inner_cells(values, others)
    return lax.slice_in_dim(values, start, start + values.shape[dim] - 2, axis=dim)


def advance(padded, crowding):
    middle = inner_cells(padded, (0, 1, 2))
    lower = [side_cells(padded, dim, 0, (0, 1, 2)) for dim in (0, 1, 2)]
    upper = [side_cells(padded, dim, 2, (0, 1, 2)) for dim in (0, 1, 2)]
    spread = lower[0] + upper[0] + lower[1] + upper[1] + lower[2] + upper[2] - 6.0 * middle
    return middle + 0.1 * spread + 0.2 * middle * (1.0 - middle * crowding)


def general(density, crowding):
    for step in range(STEPS):
        padded = with_halo(density, (("lat", 0), ("lon", 1), ("lev", 2)), 1)
        density = advance(padded, crowding)
    count = density.shape[1] * lax.axis_size("lon")
    moved = density - 1.0
    totals, squares = lax.psum(
        (jnp.sum(moved, axis=1, keepdims=True), jnp.sum(moved * moved, axis=1, keepdims=True)),
        "lon",
    )
    line_mean = 1.0 + totals / count
    centred = density - line_mean
    line_variance = squares / count - totals / count * (totals / count)
    return (centred * lax.rsqrt(line_variance + 0.0001), density)


def tree_sum(terms):
    terms = list(terms)
    while len(terms) > 1:
        terms = [sum(terms[i : i + 2][1:], terms[i]) for i in range(0, len(terms), 2)]
    return terms[0]


def kernel(lons, levs, spans, dens, crowd, out_scaled, out_dens,
           field, cap, stats, peers, load_sem, edge_sem, face_send, face_recv,
           lon_send, lon_recv, lev_send, lev_recv, stat_send, stat_recv):
    rows, cols, deep, lanes = dens.shape
    parts = len(spans)
    lat, lon, lev = lax.axis_index("lat"), lax.axis_index("lon"), lax.axis_index("lev")
    has_left, has_right = lon > 0, lon < lons - 1
    has_down, has_up = lev > 0, lev < levs - 1

    def place(r):
        return (1 - lat) * (rows - r) + lat * (r - 1)

    first = [
        pltpu.make_async_copy(
            dens.at[place(1), :, pl.ds(at, span)],
            field.at[0, 1, pl.ds(1, cols), pl.ds(PAD + at, span)],
            edge_sem.at[k])
        for k, (at, span) in enumerate(spans)
    ]
    loads = []
    for r in range(1, rows + 1):
        if r > 1:
            loads.append(pltpu.make_async_copy(
                dens.at[place(r)],
                field.at[0, r, pl.ds(1, cols), pl.ds(PAD, deep)],
                load_sem.at[0, r - 1]))
        loads.append(pltpu.make_async_copy(
            crowd.at[place(r)], cap.at[r - 1], load_sem.at[1, r - 1]))
    for copy in first + loads:
        copy.start()

    barrier = pltpu.get_barrier_semaphore()
    pl.semaphore_signal(barrier, inc=1, device_id={"lat": 1 - lat}, device_id_type=MESH)
    for j in range(1, lons):
        pl.semaphore_signal(barrier, inc=1, device_id={"lon": lax.rem(lon + j, lons)}, device_id_type=MESH)
    if levs > 1:
        @pl.when(has_down)
        def _():
            pl.semaphore_signal(barrier, inc=1, device_id={"lev": lev - 1}, device_id_type=MESH)

        @pl.when(has_up)
        def _():
            pl.semaphore_signal(barrier, inc=1, device_id={"lev": lev + 1}, device_id_type=MESH)
    pl.semaphore_wait(barrier, lons + has_down.astype(jnp.int32) + has_up.astype(jnp.int32))

    def face(t, k):
        at, span = spans[k]
        return pltpu.make_async_remote_copy(
            src_ref=field.at[t, 1, pl.ds(1, cols), pl.ds(PAD + at, span)],
            dst_ref=field.at[t, 0, pl.ds(1, cols), pl.ds(PAD + at, span)],
            send_sem=face_send.at[t, k],
            recv_sem=face_recv.at[t, k],
            device_id={"lat": 1 - lat},
            device_id_type=MESH,
        )

    def lon_side(t, right):
        own, theirs = (cols, 0) if right else (1, cols + 1)
        span = pl.ds(1, rows)
        return pltpu.make_async_remote_copy(
            src_ref=field.at[t, span, own, pl.ds(PAD, deep)],
            dst_ref=field.at[t, span, theirs, pl.ds(PAD, deep)],
            send_sem=lon_send.at[t, int(right)],
            recv_sem=lon_recv.at[t, int(right)],
            device_id={"lon": lon + 1 if right else lon - 1},
            device_id_type=MESH,
        )

    def lev_side(t, up):
        own, theirs = (PAD + deep - 1, PAD - 1) if up else (PAD, PAD + deep)
        span = (pl.ds(1, rows), pl.ds(1, cols))
        return pltpu.make_async_remote_copy(
            src_ref=field.at[t, span[0], span[1], pl.ds(own, 1)],
            dst_ref=field.at[t, span[0], span[1], pl.ds(theirs, 1)],
            send_sem=lev_send.at[t, int(up)],
            recv_sem=lev_recv.at[t, int(up)],
            device_id={"lev": lev + 1 if up else lev - 1},
            device_id_type=MESH,
        )

    def sides(t, act):
        if lons > 1:
            pl.when(has_right)(lambda: act(lon_side(t, True), 1))
            pl.when(has_left)(lambda: act(lon_side(t, False), 0))
        if levs > 1:
            pl.when(has_up)(lambda: act(lev_side(t, True), 1))
            pl.when(has_down)(lambda: act(lev_side(t, False), 0))

    def start_sides(t):
        sides(t, lambda copy, _: copy.start())

    def wait_sides_sent(t):
        sides(t, lambda copy, _: copy.wait_send())

    def wait_sides(t):
        if lons > 1:
            pl.when(has_left)(lambda: lon_side(t, True).wait_recv())
            pl.when(has_right)(lambda: lon_side(t, False).wait_recv())
        if levs > 1:
            pl.when(has_down)(lambda: lev_side(t, True).wait_recv())
            pl.when(has_up)(lambda: lev_side(t, False).wait_recv())

    def stat(part, j):
        if part < parts:
            pick = (0, slice(None), pl.ds(*spans[part]))
        else:
            pick = (pl.ds(1, rows - 1),)
        return pltpu.make_async_remote_copy(
            src_ref=stats.at[pick],
            dst_ref=peers.at[(j - 1,) + pick],
            send_sem=stat_send.at[part, j - 1],
            recv_sem=stat_recv.at[part, j - 1],
            device_id={"lon": lax.rem(lon + j, lons)},
            device_id_type=MESH,
        )

    for k in range(parts):
        first[k].wait()
        face(0, k).start()

    def clear_cols(at):
        for t in range(STEPS):
            def row(i, _, t=t):
                field[t, i, at, pl.ds(PAD, deep)] = jnp.zeros((deep, lanes), jnp.float32)
                return 0
            lax.fori_loop(1, rows + 1, row, 0)

    def clear_level(at):
        for t in range(STEPS):
            def row(i, _, t=t):
                def col(c, _):
                    field[t, i, c, pl.ds(at, PAD)] = jnp.zeros((PAD, lanes), jnp.float32)
                    return 0
                return lax.fori_loop(1, cols + 1, col, 0)
            lax.fori_loop(1, rows + 1, row, 0)

    pl.when(jnp.logical_not(has_left))(lambda: clear_cols(0))
    pl.when(jnp.logical_not(has_right))(lambda: clear_cols(cols + 1))
    pl.when(jnp.logical_not(has_down))(lambda: clear_level(0))
    pl.when(jnp.logical_not(has_up))(lambda: clear_level(PAD + deep))

    for copy in loads:
        copy.wait()
    start_sides(0)

    def cell(t, r, c, at, span, last):
        here = field[t, r, c, pl.ds(PAD + at, span)]
        near = (field[t, r, c - 1, pl.ds(PAD + at, span)] + field[t, r, c + 1, pl.ds(PAD + at, span)])
        near += (field[t, r, c, pl.ds(PAD - 1 + at, span)] + field[t, r, c, pl.ds(PAD + 1 + at, span)])
        near += field[t, r - 1, c, pl.ds(PAD + at, span)]
        if not last:
            near += field[t, r + 1, c, pl.ds(PAD + at, span)]
        limit = cap[r - 1, c - 1, pl.ds(at, span)]
        return here * (0.6 - 0.2 * (here * limit)) + 0.1 * near

    def advance_row(t, r, at, span, last):
        def col(c, _):
            field[t + 1, r, c, pl.ds(PAD + at, span)] = cell(t, r, c, at, span, last)
            return 0
        lax.fori_loop(1, cols + 1, col, 0)

    for t in range(STEPS - 1):
        wait_sides(t)

        def inner(r, _, t=t):
            advance_row(t, r, 0, deep, False)
            return 0

        lax.fori_loop(2, rows, inner, 0)
        advance_row(t, rows, 0, deep, True)
        for k in range(parts):
            face(t, k).wait_recv()
            advance_row(t, 1, *spans[k], False)
            face(t + 1, k).start()
        start_sides(t + 1)

    t = STEPS - 1
    wait_sides(t)

    def finish(r, at, last):
        values = [cell(t, r, c, at, 8, last) for c in range(1, cols + 1)]
        for c in range(cols):
            out_dens[place(r), c, pl.ds(at, 8)] = values[c]
        total = tree_sum(values)
        mean = total * (1.0 / cols)
        stats[r - 1, 0, pl.ds(at, 8)] = total
        stats[r - 1, 1, pl.ds(at, 8)] = tree_sum([(v - mean) * (v - mean) for v in values])

    def scale(r, at):
        pair = [(stats[r - 1, 0, pl.ds(at, 8)], stats[r - 1, 1, pl.ds(at, 8)])]
        for j in range(lons - 1):
            pair.append((peers[j, r - 1, 0, pl.ds(at, 8)], peers[j, r - 1, 1, pl.ds(at, 8)]))
        count = cols * lons
        mean = tree_sum([p[0] for p in pair]) * (1.0 / count)
        square = tree_sum([p[1] + cols * (p[0] * (1.0 / cols) - mean) ** 2 for p in pair])
        gain = lax.rsqrt(square * (1.0 / count) + 0.0001)
        for c in range(cols):
            out_scaled[place(r), c, pl.ds(at, 8)] = (out_dens[place(r), c, pl.ds(at, 8)] - mean) * gain

    def tiles(first, many, act):
        def tile(i, _):
            act(pl.multiple_of(i * 8, 8))
            return 0
        lax.fori_loop(first // 8, (first + many) // 8, tile, 0)

    def each_inner(act):
        def row(r, _):
            tiles(0, deep, lambda at: act(r, at))
            return 0
        lax.fori_loop(2, rows, row, 0)

    each_inner(lambda r, at: finish(r, at, False))
    tiles(0, deep, lambda at: finish(rows, at, True))
    for j in range(1, lons):
        stat(parts, j).start()
    for k in range(parts):
        face(t, k).wait_recv()
        tiles(*spans[k], lambda at: finish(1, at, False))
        for j in range(1, lons):
            stat(k, j).start()
        if k == 0:
            for j in range(1, lons):
                stat(parts, j).wait_recv()
            each_inner(scale)
            tiles(0, deep, lambda at: scale(rows, at))
        else:
            for j in range(1, lons):
                stat(k - 1, j).wait_recv()
            tiles(*spans[k - 1], lambda at: scale(1, at))
    for s in range(STEPS):
        for k in range(parts):
            face(s, k).wait_send()
        wait_sides_sent(s)
    for j in range(1, lons):
        stat(parts - 1, j).wait_recv()
    tiles(*spans[parts - 1], lambda at: scale(1, at))
    for j in range(1, lons):
        for part in range(parts + 1):
            stat(part, j).wait_send()


def writer(scaled, dens, out_scaled, out_dens, sems):
    copies = []
    for i, (src, dst) in enumerate(((scaled, out_scaled), (dens, out_dens))):
        for r in range(src.shape[0]):
            copies.append(pltpu.make_async_copy(src.at[r], dst.at[r], sems.at[i, r]))
    for copy in copies:
        copy.start()
    for copy in copies:
        copy.wait()


def written(scaled, dens):
    out = jax.ShapeDtypeStruct(dens.shape, dens.dtype)
    return pl.pallas_call(
        writer,
        out_shape=(out, out),
        in_specs=[pl.BlockSpec(memory_space=pltpu.VMEM)] * 2,
        out_specs=[pl.BlockSpec(memory_space=pl.ANY)] * 2,
        scratch_shapes=[pltpu.SemaphoreType.DMA((2, dens.shape[0]))],
        compiler_params=pltpu.CompilerParams(vmem_limit_bytes=2**20),
    )(
        pltpu.with_memory_space_constraint(scaled, pltpu.VMEM),
        pltpu.with_memory_space_constraint(dens, pltpu.VMEM),
    )


def one_kernel(lons, levs, density, crowding):
    rows, cols, deep, lanes = density.shape
    quarter = deep // 4
    spans = [(k * quarter, quarter) for k in range(4)]
    if quarter > 8:
        spans[3:] = [(3 * quarter, quarter - 8), (deep - 8, 8)]
    parts = len(spans)
    sem = pltpu.SemaphoreType.DMA
    peers = max(lons - 1, 1)
    out = pltpu.VMEM(density.shape, jnp.float32)
    return pl.pallas_call(
        functools.partial(kernel, lons, levs, spans),
        out_shape=(out, out),
        in_specs=[pl.BlockSpec(memory_space=pl.ANY)] * 2,
        out_specs=[pl.BlockSpec(memory_space=pltpu.VMEM)] * 2,
        scratch_shapes=[
            pltpu.VMEM((STEPS, rows + 1, cols + 2, deep + 2 * PAD, lanes), jnp.float32),
            pltpu.VMEM((rows, cols, deep, lanes), jnp.float32),
            pltpu.VMEM((rows, 2, deep, lanes), jnp.float32),
            pltpu.VMEM((peers, rows, 2, deep, lanes), jnp.float32),
            sem((2, rows)),
            sem((parts,)),
            sem((STEPS, parts)),
            sem((STEPS, parts)),
            sem((STEPS, 2)),
            sem((STEPS, 2)),
            sem((STEPS, 2)),
            sem((STEPS, 2)),
            sem((parts + 1, peers)),
            sem((parts + 1, peers)),
        ],
        compiler_params=pltpu.CompilerParams(
            collective_id=0, has_side_effects=True, vmem_limit_bytes=VMEM_LIMIT
        ),
    )(density, crowding)


VMEM_LIMIT = 44 * 2**20


def solution(mesh):
    lats, lons, levs = mesh.shape["lat"], mesh.shape["lon"], mesh.shape["lev"]

    def shards(density, crowding):
        rows, cols, deep, lanes = density.shape
        words = lanes * (
            STEPS * (rows + 1) * (cols + 2) * (deep + 2 * PAD)
            + 3 * rows * cols * deep
            + 2 * lons * rows * deep
        )
        fits = lats == 2 and rows > 1 and lanes == 128 and deep % 32 == 0 and 4 * words < VMEM_LIMIT
        if fits:
            return tuple(written(*one_kernel(lons, levs, density, crowding)))
        return general(density, crowding)

    spec = P(("trial", "lat"), "lon", "lev", None)
    return jax.shard_map(
        shards, mesh=mesh, in_specs=(spec, spec), out_specs=(spec, spec), check_vma=False
    )
```

```python
import functools

import jax
import jax.numpy as jnp
from jax import lax
from jax.experimental import pallas as pl
from jax.experimental.pallas import tpu as pltpu
from jax.sharding import PartitionSpec as P

STEPS = 4
PAD = 8
MESH = pl.DeviceIdType.MESH


def with_halo(cells, sides, width):
    for axis, dim in sides:
        count = lax.axis_size(axis)
        ends = count - 1
        head = lax.slice_in_dim(cells, 0, width, axis=dim)
        tail = lax.slice_in_dim(cells, cells.shape[dim] - width, cells.shape[dim], axis=dim)
        cells = jnp.concatenate(
            [
                lax.ppermute(tail, axis, [(i, (i + 1) % count) for i in range(ends)]),
                cells,
                lax.ppermute(head, axis, [((i + 1) % count, i) for i in range(ends)]),
            ],
            axis=dim,
        )
    return cells


def inner_cells(values, dims):
    for dim in dims:
        values = lax.slice_in_dim(values, 1, values.shape[dim] - 1, axis=dim)
    return values


def side_cells(values, dim, start, dims):
    others = [other for other in dims if other != dim]
    values = inner_cells(values, others)
    return lax.slice_in_dim(values, start, start + values.shape[dim] - 2, axis=dim)


def advance(padded, crowding):
    middle = inner_cells(padded, (0, 1, 2))
    lower = [side_cells(padded, dim, 0, (0, 1, 2)) for dim in (0, 1, 2)]
    upper = [side_cells(padded, dim, 2, (0, 1, 2)) for dim in (0, 1, 2)]
    spread = lower[0] + upper[0] + lower[1] + upper[1] + lower[2] + upper[2] - 6.0 * middle
    return middle + 0.1 * spread + 0.2 * middle * (1.0 - middle * crowding)


def general(density, crowding):
    for step in range(STEPS):
        padded = with_halo(density, (("lat", 0), ("lon", 1), ("lev", 2)), 1)
        density = advance(padded, crowding)
    count = density.shape[1] * lax.axis_size("lon")
    moved = density - 1.0
    totals, squares = lax.psum(
        (jnp.sum(moved, axis=1, keepdims=True), jnp.sum(moved * moved, axis=1, keepdims=True)),
        "lon",
    )
    line_mean = 1.0 + totals / count
    centred = density - line_mean
    line_variance = squares / count - totals / count * (totals / count)
    return (centred * lax.rsqrt(line_variance + 0.0001), density)


def tree_sum(terms):
    terms = list(terms)
    while len(terms) > 1:
        terms = [sum(terms[i : i + 2][1:], terms[i]) for i in range(0, len(terms), 2)]
    return terms[0]


def kernel(lons, levs, coarse, fine, dens, crowd, out_scaled, out_dens,
           field, cap, stats, peers, load_sem, edge_sem, face_send, face_recv,
           lon_send, lon_recv, lev_send, lev_recv, stat_send, stat_recv):
    rows, cols, deep, lanes = dens.shape
    spans, parts = fine, len(fine)
    lat, lon, lev = lax.axis_index("lat"), lax.axis_index("lon"), lax.axis_index("lev")
    has_left, has_right = lon > 0, lon < lons - 1
    has_down, has_up = lev > 0, lev < levs - 1

    def place(r):
        return (1 - lat) * (rows - r) + lat * (r - 1)

    first = [
        pltpu.make_async_copy(
            dens.at[place(1), :, pl.ds(at, span)],
            field.at[0, 1, pl.ds(1, cols), pl.ds(PAD + at, span)],
            edge_sem.at[k])
        for k, (at, span) in enumerate(coarse)
    ]
    loads = []
    for r in range(1, rows + 1):
        if r > 1:
            loads.append(pltpu.make_async_copy(
                dens.at[place(r)],
                field.at[0, r, pl.ds(1, cols), pl.ds(PAD, deep)],
                load_sem.at[0, r - 1]))
        loads.append(pltpu.make_async_copy(
            crowd.at[place(r)], cap.at[r - 1], load_sem.at[1, r - 1]))
    for copy in first + loads:
        copy.start()

    barrier = pltpu.get_barrier_semaphore()
    pl.semaphore_signal(barrier, inc=1, device_id={"lat": 1 - lat}, device_id_type=MESH)
    for j in range(1, lons):
        pl.semaphore_signal(barrier, inc=1, device_id={"lon": lax.rem(lon + j, lons)}, device_id_type=MESH)
    if levs > 1:
        @pl.when(has_down)
        def _():
            pl.semaphore_signal(barrier, inc=1, device_id={"lev": lev - 1}, device_id_type=MESH)

        @pl.when(has_up)
        def _():
            pl.semaphore_signal(barrier, inc=1, device_id={"lev": lev + 1}, device_id_type=MESH)
    pl.semaphore_wait(barrier, lons + has_down.astype(jnp.int32) + has_up.astype(jnp.int32))

    def chunks(t):
        return fine if t == STEPS - 1 else coarse

    def face(t, k):
        at, span = chunks(t)[k]
        return pltpu.make_async_remote_copy(
            src_ref=field.at[t, 1, pl.ds(1, cols), pl.ds(PAD + at, span)],
            dst_ref=field.at[t, 0, pl.ds(1, cols), pl.ds(PAD + at, span)],
            send_sem=face_send.at[t, k],
            recv_sem=face_recv.at[t, k],
            device_id={"lat": 1 - lat},
            device_id_type=MESH,
        )

    def lon_side(t, right):
        own, theirs = (cols, 0) if right else (1, cols + 1)
        span = pl.ds(1, rows)
        return pltpu.make_async_remote_copy(
            src_ref=field.at[t, span, own, pl.ds(PAD, deep)],
            dst_ref=field.at[t, span, theirs, pl.ds(PAD, deep)],
            send_sem=lon_send.at[t, int(right)],
            recv_sem=lon_recv.at[t, int(right)],
            device_id={"lon": lon + 1 if right else lon - 1},
            device_id_type=MESH,
        )

    def lev_side(t, up):
        own, theirs = (PAD + deep - 1, PAD - 1) if up else (PAD, PAD + deep)
        span = (pl.ds(1, rows), pl.ds(1, cols))
        return pltpu.make_async_remote_copy(
            src_ref=field.at[t, span[0], span[1], pl.ds(own, 1)],
            dst_ref=field.at[t, span[0], span[1], pl.ds(theirs, 1)],
            send_sem=lev_send.at[t, int(up)],
            recv_sem=lev_recv.at[t, int(up)],
            device_id={"lev": lev + 1 if up else lev - 1},
            device_id_type=MESH,
        )

    def sides(t, act):
        if lons > 1:
            pl.when(has_right)(lambda: act(lon_side(t, True), 1))
            pl.when(has_left)(lambda: act(lon_side(t, False), 0))
        if levs > 1:
            pl.when(has_up)(lambda: act(lev_side(t, True), 1))
            pl.when(has_down)(lambda: act(lev_side(t, False), 0))

    def start_sides(t):
        sides(t, lambda copy, _: copy.start())

    def wait_sides_sent(t):
        sides(t, lambda copy, _: copy.wait_send())

    def wait_sides(t):
        if lons > 1:
            pl.when(has_left)(lambda: lon_side(t, True).wait_recv())
            pl.when(has_right)(lambda: lon_side(t, False).wait_recv())
        if levs > 1:
            pl.when(has_down)(lambda: lev_side(t, True).wait_recv())
            pl.when(has_up)(lambda: lev_side(t, False).wait_recv())

    def stat(part, j):
        if part < parts:
            pick = (0, slice(None), pl.ds(*spans[part]))
        else:
            pick = (pl.ds(1, rows - 1),)
        return pltpu.make_async_remote_copy(
            src_ref=stats.at[pick],
            dst_ref=peers.at[(j - 1,) + pick],
            send_sem=stat_send.at[part, j - 1],
            recv_sem=stat_recv.at[part, j - 1],
            device_id={"lon": lax.rem(lon + j, lons)},
            device_id_type=MESH,
        )

    for k in range(len(coarse)):
        first[k].wait()
        face(0, k).start()

    def clear_cols(at):
        for t in range(STEPS):
            def row(i, _, t=t):
                field[t, i, at, pl.ds(PAD, deep)] = jnp.zeros((deep, lanes), jnp.float32)
                return 0
            lax.fori_loop(1, rows + 1, row, 0)

    def clear_level(at):
        for t in range(STEPS):
            def row(i, _, t=t):
                def col(c, _):
                    field[t, i, c, pl.ds(at, PAD)] = jnp.zeros((PAD, lanes), jnp.float32)
                    return 0
                return lax.fori_loop(1, cols + 1, col, 0)
            lax.fori_loop(1, rows + 1, row, 0)

    pl.when(jnp.logical_not(has_left))(lambda: clear_cols(0))
    pl.when(jnp.logical_not(has_right))(lambda: clear_cols(cols + 1))
    pl.when(jnp.logical_not(has_down))(lambda: clear_level(0))
    pl.when(jnp.logical_not(has_up))(lambda: clear_level(PAD + deep))

    for copy in loads:
        copy.wait()
    start_sides(0)

    def cell(t, r, c, at, span, last):
        here = field[t, r, c, pl.ds(PAD + at, span)]
        near = (field[t, r, c - 1, pl.ds(PAD + at, span)] + field[t, r, c + 1, pl.ds(PAD + at, span)])
        near += (field[t, r, c, pl.ds(PAD - 1 + at, span)] + field[t, r, c, pl.ds(PAD + 1 + at, span)])
        near += field[t, r - 1, c, pl.ds(PAD + at, span)]
        if not last:
            near += field[t, r + 1, c, pl.ds(PAD + at, span)]
        limit = cap[r - 1, c - 1, pl.ds(at, span)]
        return here * (0.6 - 0.2 * (here * limit)) + 0.1 * near

    def advance_row(t, r, at, span, last):
        def col(c, _):
            field[t + 1, r, c, pl.ds(PAD + at, span)] = cell(t, r, c, at, span, last)
            return 0
        lax.fori_loop(1, cols + 1, col, 0)

    for t in range(STEPS - 1):
        wait_sides(t)

        def inner(r, _, t=t):
            advance_row(t, r, 0, deep, False)
            return 0

        lax.fori_loop(2, rows, inner, 0)
        advance_row(t, rows, 0, deep, True)
        for k in range(len(coarse)):
            face(t, k).wait_recv()
            advance_row(t, 1, *coarse[k], False)
            for j, (at, _) in enumerate(chunks(t + 1)):
                if coarse[k][0] <= at < sum(coarse[k]):
                    face(t + 1, j).start()
        start_sides(t + 1)

    t = STEPS - 1
    wait_sides(t)

    def finish(r, at, last):
        values = [cell(t, r, c, at, 8, last) for c in range(1, cols + 1)]
        for c in range(cols):
            out_dens[place(r), c, pl.ds(at, 8)] = values[c]
        total = tree_sum(values)
        mean = total * (1.0 / cols)
        stats[r - 1, 0, pl.ds(at, 8)] = total
        stats[r - 1, 1, pl.ds(at, 8)] = tree_sum([(v - mean) * (v - mean) for v in values])

    def scale(r, at):
        pair = [(stats[r - 1, 0, pl.ds(at, 8)], stats[r - 1, 1, pl.ds(at, 8)])]
        for j in range(lons - 1):
            pair.append((peers[j, r - 1, 0, pl.ds(at, 8)], peers[j, r - 1, 1, pl.ds(at, 8)]))
        count = cols * lons
        mean = tree_sum([p[0] for p in pair]) * (1.0 / count)
        square = tree_sum([p[1] + cols * (p[0] * (1.0 / cols) - mean) ** 2 for p in pair])
        gain = lax.rsqrt(square * (1.0 / count) + 0.0001)
        for c in range(cols):
            out_scaled[place(r), c, pl.ds(at, 8)] = (out_dens[place(r), c, pl.ds(at, 8)] - mean) * gain

    def tiles(first, many, act):
        def tile(i, _):
            act(pl.multiple_of(i * 8, 8))
            return 0
        lax.fori_loop(first // 8, (first + many) // 8, tile, 0)

    def each_inner(act):
        def row(r, _):
            tiles(0, deep, lambda at: act(r, at))
            return 0
        lax.fori_loop(2, rows, row, 0)

    each_inner(lambda r, at: finish(r, at, False))
    tiles(0, deep, lambda at: finish(rows, at, True))
    for j in range(1, lons):
        stat(parts, j).start()
    for k in range(parts):
        face(t, k).wait_recv()
        tiles(*spans[k], lambda at: finish(1, at, False))
        for j in range(1, lons):
            stat(k, j).start()
        if k == 0:
            for j in range(1, lons):
                stat(parts, j).wait_recv()
            each_inner(scale)
            tiles(0, deep, lambda at: scale(rows, at))
        else:
            for j in range(1, lons):
                stat(k - 1, j).wait_recv()
            tiles(*spans[k - 1], lambda at: scale(1, at))
    for s in range(STEPS):
        for k in range(len(chunks(s))):
            face(s, k).wait_send()
        wait_sides_sent(s)
    for j in range(1, lons):
        stat(parts - 1, j).wait_recv()
    tiles(*spans[parts - 1], lambda at: scale(1, at))
    for j in range(1, lons):
        for part in range(parts + 1):
            stat(part, j).wait_send()


def writer(scaled, dens, out_scaled, out_dens, sems):
    copies = []
    for i, (src, dst) in enumerate(((scaled, out_scaled), (dens, out_dens))):
        for r in range(src.shape[0]):
            copies.append(pltpu.make_async_copy(src.at[r], dst.at[r], sems.at[i, r]))
    for copy in copies:
        copy.start()
    for copy in copies:
        copy.wait()


def written(scaled, dens):
    out = jax.ShapeDtypeStruct(dens.shape, dens.dtype)
    return pl.pallas_call(
        writer,
        out_shape=(out, out),
        in_specs=[pl.BlockSpec(memory_space=pltpu.VMEM)] * 2,
        out_specs=[pl.BlockSpec(memory_space=pl.ANY)] * 2,
        scratch_shapes=[pltpu.SemaphoreType.DMA((2, dens.shape[0]))],
        compiler_params=pltpu.CompilerParams(vmem_limit_bytes=2**20),
    )(
        pltpu.with_memory_space_constraint(scaled, pltpu.VMEM),
        pltpu.with_memory_space_constraint(dens, pltpu.VMEM),
    )


def one_kernel(lons, levs, density, crowding):
    rows, cols, deep, lanes = density.shape
    half = deep // 2
    coarse = [(0, half), (half, half)]
    fine = coarse[:1] + [(half, half - 8), (deep - 8, 8)]
    parts = len(fine)
    sem = pltpu.SemaphoreType.DMA
    peers = max(lons - 1, 1)
    out = pltpu.VMEM(density.shape, jnp.float32)
    return pl.pallas_call(
        functools.partial(kernel, lons, levs, coarse, fine),
        out_shape=(out, out),
        in_specs=[pl.BlockSpec(memory_space=pl.ANY)] * 2,
        out_specs=[pl.BlockSpec(memory_space=pltpu.VMEM)] * 2,
        scratch_shapes=[
            pltpu.VMEM((STEPS, rows + 1, cols + 2, deep + 2 * PAD, lanes), jnp.float32),
            pltpu.VMEM((rows, cols, deep, lanes), jnp.float32),
            pltpu.VMEM((rows, 2, deep, lanes), jnp.float32),
            pltpu.VMEM((peers, rows, 2, deep, lanes), jnp.float32),
            sem((2, rows)),
            sem((len(coarse),)),
            sem((STEPS, parts)),
            sem((STEPS, parts)),
            sem((STEPS, 2)),
            sem((STEPS, 2)),
            sem((STEPS, 2)),
            sem((STEPS, 2)),
            sem((parts + 1, peers)),
            sem((parts + 1, peers)),
        ],
        compiler_params=pltpu.CompilerParams(
            collective_id=0, has_side_effects=True, vmem_limit_bytes=VMEM_LIMIT
        ),
    )(density, crowding)


VMEM_LIMIT = 44 * 2**20


def solution(mesh):
    lats, lons, levs = mesh.shape["lat"], mesh.shape["lon"], mesh.shape["lev"]

    def shards(density, crowding):
        rows, cols, deep, lanes = density.shape
        words = lanes * (
            STEPS * (rows + 1) * (cols + 2) * (deep + 2 * PAD)
            + 3 * rows * cols * deep
            + 2 * lons * rows * deep
        )
        fits = lats == 2 and rows > 1 and lanes == 128 and deep % 32 == 0 and 4 * words < VMEM_LIMIT
        if fits:
            return tuple(written(*one_kernel(lons, levs, density, crowding)))
        return general(density, crowding)

    spec = P(("trial", "lat"), "lon", "lev", None)
    return jax.shard_map(
        shards, mesh=mesh, in_specs=(spec, spec), out_specs=(spec, spec), check_vma=False
    )
```

```python
import functools

import jax
import jax.numpy as jnp
from jax import lax
from jax.experimental import pallas as pl
from jax.experimental.pallas import tpu as pltpu
from jax.sharding import PartitionSpec as P

STEPS = 4
PAD = 8
MESH = pl.DeviceIdType.MESH


def with_halo(cells, sides, width):
    for axis, dim in sides:
        count = lax.axis_size(axis)
        ends = count - 1
        head = lax.slice_in_dim(cells, 0, width, axis=dim)
        tail = lax.slice_in_dim(cells, cells.shape[dim] - width, cells.shape[dim], axis=dim)
        cells = jnp.concatenate(
            [
                lax.ppermute(tail, axis, [(i, (i + 1) % count) for i in range(ends)]),
                cells,
                lax.ppermute(head, axis, [((i + 1) % count, i) for i in range(ends)]),
            ],
            axis=dim,
        )
    return cells


def inner_cells(values, dims):
    for dim in dims:
        values = lax.slice_in_dim(values, 1, values.shape[dim] - 1, axis=dim)
    return values


def side_cells(values, dim, start, dims):
    others = [other for other in dims if other != dim]
    values = inner_cells(values, others)
    return lax.slice_in_dim(values, start, start + values.shape[dim] - 2, axis=dim)


def advance(padded, crowding):
    middle = inner_cells(padded, (0, 1, 2))
    lower = [side_cells(padded, dim, 0, (0, 1, 2)) for dim in (0, 1, 2)]
    upper = [side_cells(padded, dim, 2, (0, 1, 2)) for dim in (0, 1, 2)]
    spread = lower[0] + upper[0] + lower[1] + upper[1] + lower[2] + upper[2] - 6.0 * middle
    return middle + 0.1 * spread + 0.2 * middle * (1.0 - middle * crowding)


def general(density, crowding):
    for step in range(STEPS):
        padded = with_halo(density, (("lat", 0), ("lon", 1), ("lev", 2)), 1)
        density = advance(padded, crowding)
    count = density.shape[1] * lax.axis_size("lon")
    moved = density - 1.0
    totals, squares = lax.psum(
        (jnp.sum(moved, axis=1, keepdims=True), jnp.sum(moved * moved, axis=1, keepdims=True)),
        "lon",
    )
    line_mean = 1.0 + totals / count
    centred = density - line_mean
    line_variance = squares / count - totals / count * (totals / count)
    return (centred * lax.rsqrt(line_variance + 0.0001), density)


def tree_sum(terms):
    terms = list(terms)
    while len(terms) > 1:
        terms = [sum(terms[i : i + 2][1:], terms[i]) for i in range(0, len(terms), 2)]
    return terms[0]


def kernel(lons, levs, coarse, fine, dens, crowd, out_scaled, out_dens,
           field, cap, stats, peers, load_sem, edge_sem, face_send, face_recv,
           lon_send, lon_recv, lev_send, lev_recv, stat_send, stat_recv):
    rows, cols, deep, lanes = dens.shape
    spans, parts = fine, len(fine)
    lat, lon, lev = lax.axis_index("lat"), lax.axis_index("lon"), lax.axis_index("lev")
    has_left, has_right = lon > 0, lon < lons - 1
    has_down, has_up = lev > 0, lev < levs - 1

    def place(r):
        return (1 - lat) * (rows - r) + lat * (r - 1)

    first = [
        pltpu.make_async_copy(
            dens.at[place(1), :, pl.ds(at, span)],
            field.at[0, 1, pl.ds(1, cols), pl.ds(PAD + at, span)],
            edge_sem.at[k])
        for k, (at, span) in enumerate(coarse)
    ]
    loads = []
    for r in range(1, rows + 1):
        if r > 1:
            loads.append(pltpu.make_async_copy(
                dens.at[place(r)],
                field.at[0, r, pl.ds(1, cols), pl.ds(PAD, deep)],
                load_sem.at[0, r - 1]))
        loads.append(pltpu.make_async_copy(
            crowd.at[place(r)], cap.at[r - 1], load_sem.at[1, r - 1]))
    for copy in first + loads:
        copy.start()

    barrier = pltpu.get_barrier_semaphore()
    pl.semaphore_signal(barrier, inc=1, device_id={"lat": 1 - lat}, device_id_type=MESH)
    for j in range(1, lons):
        pl.semaphore_signal(barrier, inc=1, device_id={"lon": lax.rem(lon + j, lons)}, device_id_type=MESH)
    if levs > 1:
        @pl.when(has_down)
        def _():
            pl.semaphore_signal(barrier, inc=1, device_id={"lev": lev - 1}, device_id_type=MESH)

        @pl.when(has_up)
        def _():
            pl.semaphore_signal(barrier, inc=1, device_id={"lev": lev + 1}, device_id_type=MESH)
    pl.semaphore_wait(barrier, lons + has_down.astype(jnp.int32) + has_up.astype(jnp.int32))

    def chunks(t):
        return fine if t == STEPS - 1 else coarse

    def face(t, k):
        at, span = chunks(t)[k]
        return pltpu.make_async_remote_copy(
            src_ref=field.at[t, 1, pl.ds(1, cols), pl.ds(PAD + at, span)],
            dst_ref=field.at[t, 0, pl.ds(1, cols), pl.ds(PAD + at, span)],
            send_sem=face_send.at[t, k],
            recv_sem=face_recv.at[t, k],
            device_id={"lat": 1 - lat},
            device_id_type=MESH,
        )

    def lon_side(t, right):
        own, theirs = (cols, 0) if right else (1, cols + 1)
        span = pl.ds(1, rows)
        return pltpu.make_async_remote_copy(
            src_ref=field.at[t, span, own, pl.ds(PAD, deep)],
            dst_ref=field.at[t, span, theirs, pl.ds(PAD, deep)],
            send_sem=lon_send.at[t, int(right)],
            recv_sem=lon_recv.at[t, int(right)],
            device_id={"lon": lon + 1 if right else lon - 1},
            device_id_type=MESH,
        )

    def lev_side(t, up):
        own, theirs = (PAD + deep - 1, PAD - 1) if up else (PAD, PAD + deep)
        span = (pl.ds(1, rows), pl.ds(1, cols))
        return pltpu.make_async_remote_copy(
            src_ref=field.at[t, span[0], span[1], pl.ds(own, 1)],
            dst_ref=field.at[t, span[0], span[1], pl.ds(theirs, 1)],
            send_sem=lev_send.at[t, int(up)],
            recv_sem=lev_recv.at[t, int(up)],
            device_id={"lev": lev + 1 if up else lev - 1},
            device_id_type=MESH,
        )

    def sides(t, act):
        if lons > 1:
            pl.when(has_right)(lambda: act(lon_side(t, True), 1))
            pl.when(has_left)(lambda: act(lon_side(t, False), 0))
        if levs > 1:
            pl.when(has_up)(lambda: act(lev_side(t, True), 1))
            pl.when(has_down)(lambda: act(lev_side(t, False), 0))

    def start_sides(t):
        sides(t, lambda copy, _: copy.start())

    def wait_sides_sent(t):
        sides(t, lambda copy, _: copy.wait_send())

    def wait_sides(t):
        if lons > 1:
            pl.when(has_left)(lambda: lon_side(t, True).wait_recv())
            pl.when(has_right)(lambda: lon_side(t, False).wait_recv())
        if levs > 1:
            pl.when(has_down)(lambda: lev_side(t, True).wait_recv())
            pl.when(has_up)(lambda: lev_side(t, False).wait_recv())

    def stat(part, j):
        if part < parts:
            pick = (0, slice(None), pl.ds(*spans[part]))
        else:
            pick = (pl.ds(1, rows - 1),)
        return pltpu.make_async_remote_copy(
            src_ref=stats.at[pick],
            dst_ref=peers.at[(j - 1,) + pick],
            send_sem=stat_send.at[part, j - 1],
            recv_sem=stat_recv.at[part, j - 1],
            device_id={"lon": lax.rem(lon + j, lons)},
            device_id_type=MESH,
        )

    for k in range(len(coarse)):
        first[k].wait()
        face(0, k).start()

    def clear_cols(at):
        for t in range(STEPS):
            def row(i, _, t=t):
                field[t, i, at, pl.ds(PAD, deep)] = jnp.zeros((deep, lanes), jnp.float32)
                return 0
            lax.fori_loop(1, rows + 1, row, 0)

    def clear_level(at):
        for t in range(STEPS):
            def row(i, _, t=t):
                def col(c, _):
                    field[t, i, c, pl.ds(at, PAD)] = jnp.zeros((PAD, lanes), jnp.float32)
                    return 0
                return lax.fori_loop(1, cols + 1, col, 0)
            lax.fori_loop(1, rows + 1, row, 0)

    pl.when(jnp.logical_not(has_left))(lambda: clear_cols(0))
    pl.when(jnp.logical_not(has_right))(lambda: clear_cols(cols + 1))
    pl.when(jnp.logical_not(has_down))(lambda: clear_level(0))
    pl.when(jnp.logical_not(has_up))(lambda: clear_level(PAD + deep))

    for copy in loads:
        copy.wait()
    start_sides(0)

    def cell(t, r, c, at, span, last):
        here = field[t, r, c, pl.ds(PAD + at, span)]
        near = (field[t, r, c - 1, pl.ds(PAD + at, span)] + field[t, r, c + 1, pl.ds(PAD + at, span)])
        near += (field[t, r, c, pl.ds(PAD - 1 + at, span)] + field[t, r, c, pl.ds(PAD + 1 + at, span)])
        near += field[t, r - 1, c, pl.ds(PAD + at, span)]
        if not last:
            near += field[t, r + 1, c, pl.ds(PAD + at, span)]
        limit = cap[r - 1, c - 1, pl.ds(at, span)]
        return here * (0.6 - 0.2 * (here * limit)) + 0.1 * near

    def advance_row(t, r, at, span, last):
        def col(c, _):
            field[t + 1, r, c, pl.ds(PAD + at, span)] = cell(t, r, c, at, span, last)
            return 0
        lax.fori_loop(1, cols + 1, col, 0)

    for t in range(STEPS - 1):
        wait_sides(t)

        def inner(r, _, t=t):
            advance_row(t, r, 0, deep, False)
            return 0

        lax.fori_loop(2, rows, inner, 0)
        advance_row(t, rows, 0, deep, True)
        for k in range(len(coarse)):
            face(t, k).wait_recv()
            advance_row(t, 1, *coarse[k], False)
            for j, (at, _) in enumerate(chunks(t + 1)):
                if coarse[k][0] <= at < sum(coarse[k]):
                    face(t + 1, j).start()
        start_sides(t + 1)

    t = STEPS - 1
    wait_sides(t)

    def finish(r, at, last):
        values = [cell(t, r, c, at, 8, last) for c in range(1, cols + 1)]
        for c in range(cols):
            out_dens[place(r), c, pl.ds(at, 8)] = values[c]
        total = tree_sum(values)
        mean = total * (1.0 / cols)
        stats[r - 1, 0, pl.ds(at, 8)] = total
        stats[r - 1, 1, pl.ds(at, 8)] = tree_sum([(v - mean) * (v - mean) for v in values])

    def scale(r, at):
        pair = [(stats[r - 1, 0, pl.ds(at, 8)], stats[r - 1, 1, pl.ds(at, 8)])]
        for j in range(lons - 1):
            pair.append((peers[j, r - 1, 0, pl.ds(at, 8)], peers[j, r - 1, 1, pl.ds(at, 8)]))
        count = cols * lons
        mean = tree_sum([p[0] for p in pair]) * (1.0 / count)
        square = tree_sum([p[1] + cols * (p[0] * (1.0 / cols) - mean) ** 2 for p in pair])
        gain = lax.rsqrt(square * (1.0 / count) + 0.0001)
        for c in range(cols):
            out_scaled[place(r), c, pl.ds(at, 8)] = (out_dens[place(r), c, pl.ds(at, 8)] - mean) * gain

    def tiles(first, many, act):
        def tile(i, _):
            act(pl.multiple_of(i * 8, 8))
            return 0
        lax.fori_loop(first // 8, (first + many) // 8, tile, 0)

    def each_inner(act):
        def row(r, _):
            tiles(0, deep, lambda at: act(r, at))
            return 0
        lax.fori_loop(2, rows, row, 0)

    each_inner(lambda r, at: finish(r, at, False))
    tiles(0, deep, lambda at: finish(rows, at, True))
    for j in range(1, lons):
        stat(parts, j).start()
    for k in range(parts):
        face(t, k).wait_recv()
        tiles(*spans[k], lambda at: finish(1, at, False))
        for j in range(1, lons):
            stat(k, j).start()
        if k == 0:
            for j in range(1, lons):
                stat(parts, j).wait_recv()
            each_inner(scale)
            tiles(0, deep, lambda at: scale(rows, at))
        else:
            for j in range(1, lons):
                stat(k - 1, j).wait_recv()
            tiles(*spans[k - 1], lambda at: scale(1, at))
    for s in range(STEPS):
        for k in range(len(chunks(s))):
            face(s, k).wait_send()
        wait_sides_sent(s)
    for j in range(1, lons):
        stat(parts - 1, j).wait_recv()
    tiles(*spans[parts - 1], lambda at: scale(1, at))
    for j in range(1, lons):
        for part in range(parts + 1):
            stat(part, j).wait_send()


def writer(scaled, dens, out_scaled, out_dens, sems):
    copies = []
    for i, (src, dst) in enumerate(((scaled, out_scaled), (dens, out_dens))):
        for r in range(src.shape[0]):
            copies.append(pltpu.make_async_copy(src.at[r], dst.at[r], sems.at[i, r]))
    for copy in copies:
        copy.start()
    for copy in copies:
        copy.wait()


def written(scaled, dens):
    out = jax.ShapeDtypeStruct(dens.shape, dens.dtype)
    return pl.pallas_call(
        writer,
        out_shape=(out, out),
        in_specs=[pl.BlockSpec(memory_space=pltpu.VMEM)] * 2,
        out_specs=[pl.BlockSpec(memory_space=pl.ANY)] * 2,
        scratch_shapes=[pltpu.SemaphoreType.DMA((2, dens.shape[0]))],
        compiler_params=pltpu.CompilerParams(vmem_limit_bytes=2**20),
    )(
        pltpu.with_memory_space_constraint(scaled, pltpu.VMEM),
        pltpu.with_memory_space_constraint(dens, pltpu.VMEM),
    )


def one_kernel(lons, levs, density, crowding):
    rows, cols, deep, lanes = density.shape
    half = deep // 2
    coarse = [(0, half), (half, half)]
    fine = coarse[:1] + [(half, half - 24), (deep - 24, 16), (deep - 8, 8)]
    parts = len(fine)
    sem = pltpu.SemaphoreType.DMA
    peers = max(lons - 1, 1)
    out = pltpu.VMEM(density.shape, jnp.float32)
    return pl.pallas_call(
        functools.partial(kernel, lons, levs, coarse, fine),
        out_shape=(out, out),
        in_specs=[pl.BlockSpec(memory_space=pl.ANY)] * 2,
        out_specs=[pl.BlockSpec(memory_space=pltpu.VMEM)] * 2,
        scratch_shapes=[
            pltpu.VMEM((STEPS, rows + 1, cols + 2, deep + 2 * PAD, lanes), jnp.float32),
            pltpu.VMEM((rows, cols, deep, lanes), jnp.float32),
            pltpu.VMEM((rows, 2, deep, lanes), jnp.float32),
            pltpu.VMEM((peers, rows, 2, deep, lanes), jnp.float32),
            sem((2, rows)),
            sem((len(coarse),)),
            sem((STEPS, parts)),
            sem((STEPS, parts)),
            sem((STEPS, 2)),
            sem((STEPS, 2)),
            sem((STEPS, 2)),
            sem((STEPS, 2)),
            sem((parts + 1, peers)),
            sem((parts + 1, peers)),
        ],
        compiler_params=pltpu.CompilerParams(
            collective_id=0, has_side_effects=True, vmem_limit_bytes=VMEM_LIMIT
        ),
    )(density, crowding)


VMEM_LIMIT = 44 * 2**20


def solution(mesh):
    lats, lons, levs = mesh.shape["lat"], mesh.shape["lon"], mesh.shape["lev"]

    def shards(density, crowding):
        rows, cols, deep, lanes = density.shape
        words = lanes * (
            STEPS * (rows + 1) * (cols + 2) * (deep + 2 * PAD)
            + 3 * rows * cols * deep
            + 2 * lons * rows * deep
        )
        fits = lats == 2 and rows > 1 and lanes == 128 and deep % 32 == 0 and deep >= 64 and 4 * words < VMEM_LIMIT
        if fits:
            return tuple(written(*one_kernel(lons, levs, density, crowding)))
        return general(density, crowding)

    spec = P(("trial", "lat"), "lon", "lev", None)
    return jax.shard_map(
        shards, mesh=mesh, in_specs=(spec, spec), out_specs=(spec, spec), check_vma=False
    )
```
